32 devices in a mesh: dp: 16 (over z, x, core), tp: 2 (over y).
Axes of the slice: x: 2, y: 2, z: 4, core: 2. Of those that a mesh axis runs over, the one named last changes fastest.
Arguments:
- hidden: bfloat16 [512, 4096], P('dp', 'tp'), may hold values from -6 to 6
- routes: int32 [512, 8], P('dp'), may hold values from 0 to 15, all different within a row; in each aligned block of 32 rows (0 to 31, 32 to 63, ...) at most 32 rows name the same one
- routing_weights: float32 [512, 8], P('dp'), may hold values from 0.05 to 1
- w_gate: bfloat16 [16, 4096, 1536], P('dp', None, 'tp'), may hold values from -0.09375 to 0.09375
- w_up: bfloat16 [16, 4096, 1536], P('dp', None, 'tp'), may hold values from -0.09375 to 0.09375
- w_down: bfloat16 [16, 1536, 4096], P('dp', 'tp'), may hold values from -0.15625 to 0.15625
- norm_gain: float32 [4096], replicated, may hold values from 0.1 to 1.9
- key_projection_weight: bfloat16 [4096, 512], P(None, 'tp'), may hold values from -0.09375 to 0.09375
- value_projection_weight: bfloat16 [4096, 512], P(None, 'tp'), may hold values from -0.09375 to 0.09375
- queries: bfloat16 [512, 8192], P('dp', 'tp'), may hold values from -128 to 128
- cached_key_rows: bfloat16 [16, 128, 512], P('dp', None, 'tp'), may hold values from -4 to 4
- cached_value_rows: bfloat16 [16, 128, 512], P('dp', None, 'tp'), may hold values from -6 to 6
- lengths: int32 [16], P('dp'), may hold values from 16 to 128
- parents: int32 [16, 32], P('dp'), may hold values from -1 to 30, as said below
Outputs:
- layer_output: bfloat16 [512, 4096], P('dp', 'tp')
- next_layer_keys: bfloat16 [512, 512], P('dp', 'tp')
- next_layer_values: bfloat16 [512, 512], P('dp', 'tp')
- attended: bfloat16 [512, 8192], P('dp', 'tp')
The draws below stay inside these ranges and needn't reach their ends.
Inputs may be any that keep to these rules, and one draw needn't show every extreme that they name: `routes`: each row names 8 different experts. In each aligned block of 32 rows (the rows of one device) no expert is named by more than 32 rows, a bound that some block reaches. `parents`: node 0 of each request is the root, with parent -1; every other node i has its parent among nodes max(0, i - 8) to i - 1.
All inputs are finite; a program needn't handle non-finite values.
Results may differ from the reference program's by a relative error of at most 0.013.
Values may be sent and summed in bfloat16 or wider, within the bound.
A program may use at most 64 MiB of HBM per device.

```python
import math
import jax
import jax.numpy as jnp
import numpy as np
from jax import lax

MODEL_WIDTH = 4096
QUERY_HEADS = 64
KEY_VALUE_HEADS = 4
HEAD_SIZE = 128
FF = 1536
TOP = 8
TREE_TOKENS = 32
CONTEXT_SLOTS = 128
EXPERTS = 16
T_DEV = 32
REQUEST_TOTAL = 16
TOKENS = 512
CAP = 32
N_DP = 16
N_TP = 2


def attention_pair(key):
    request_key_cache = jax.random.fold_in(key, 101)
    key_query = jax.random.fold_in(key, 202)
    kept_length = jnp.clip(jax.random.normal(request_key_cache, (REQUEST_TOTAL, CONTEXT_SLOTS, KEY_VALUE_HEADS, HEAD_SIZE), jnp.float32), -4.0, 4.0)
    wanted_rows = jnp.clip(jax.random.normal(key_query, (REQUEST_TOTAL, TREE_TOKENS, QUERY_HEADS, HEAD_SIZE), jnp.float32), -4.0, 4.0)
    return (kept_length.reshape(REQUEST_TOTAL, CONTEXT_SLOTS, KEY_VALUE_HEADS * HEAD_SIZE), wanted_rows.reshape(REQUEST_TOTAL * TREE_TOKENS, QUERY_HEADS * HEAD_SIZE))


def draw_queries(key, part):
    return attention_pair(key)[1].astype(jnp.bfloat16)


def draw_cached_key_rows(key, part):
    return attention_pair(key)[0].astype(jnp.bfloat16)


def draw_parents(key, part):
    position = jnp.arange(TREE_TOKENS, dtype=jnp.int32)
    lowest = jnp.maximum(position - 8, 0)
    highest = jnp.maximum(position, 1)
    picks = jax.random.randint(jax.random.fold_in(key, 303), (REQUEST_TOTAL, TREE_TOKENS), lowest, highest, dtype=jnp.int32)
    return jnp.where(position[None, :] == 0, -1, picks).astype(jnp.int32)


def set_ends(values, own_key, low, top_value):
    longest = values.shape.index(max(values.shape))
    spots = []
    for shift in (0, 1):
        where = [jax.random.randint(jax.random.fold_in(own_key, axis), (), 0, length) for axis, length in enumerate(values.shape)]
        where[longest] = (where[longest] + shift) % values.shape[longest]
        spots.append(tuple(where))
    return values.at[spots[0]].set(low).at[spots[1]].set(top_value)


def level_of(key, extent, split, smallest, high):
    loudness, own = 1.0, jax.random.fold_in(key, 6)
    for dim, blocks in split:
        heights = jnp.exp(jax.random.uniform(jax.random.fold_in(own, dim), (blocks,), jnp.float32, smallest / len(split), high / len(split)))
        loudness = loudness * jnp.repeat(heights, extent[dim] // blocks).reshape([-1 if axis == dim else 1 for axis in range(len(extent))])
    return loudness


def routed_block(key, own, number, rows, amount, top, bound, skew):
    ranking = jax.random.permutation(key, amount)
    heavy_load, usual = portions_of(amount, rows * top, bound, skew, True), portions_of(amount, rows * top, bound, skew, False)
    places = jnp.arange(amount)

    def named(sizes, turn):
        used = int((sizes > 0).sum())
        fixed = max(1, used // 4)
        shifted = fixed + (places - fixed + turn * (used - fixed)) % max(1, amount - fixed)
        return jnp.zeros((amount,), jnp.int32).at[ranking[jnp.where(places < fixed, places, shifted)]].set(jnp.asarray(sizes, jnp.int32))

    sizes = jnp.where(number % 4 == 0, named(heavy_load, number // 4), named(usual, number - number // 4 - 1))
    mixed = jax.random.permutation(jax.random.fold_in(own, 3), amount)
    source_of, taker = mixed[0:amount // 2 * 2:2], mixed[1:amount // 2 * 2:2]
    slack = jnp.minimum(sizes[source_of] - 1, bound - sizes[taker]) // 2
    slack = jnp.where((source_of == ranking[0]) | (taker == ranking[0]) | (sizes[taker] == 0), 0, jnp.maximum(slack, 0))
    shifted = jax.random.randint(jax.random.fold_in(own, 4), (amount // 2,), 0, 1 << 20) % (slack + 1)
    sizes = sizes.at[source_of].add(-shifted).at[taker].add(shifted)
    labels = jnp.searchsorted(jnp.cumsum(sizes), jnp.arange(rows * top), side="right").astype(jnp.int32)
    grid = labels.reshape(top, rows).T
    grid = grid[jax.random.permutation(jax.random.fold_in(own, 1), rows)]
    turn = jax.random.randint(jax.random.fold_in(own, 2), (rows, 1), 0, top)
    return jnp.take_along_axis(grid, (jnp.arange(top)[None, :] + turn) % top, axis=1)


def portions_of(number_of, total, reach, slope, full):
    weights = [(1 << 20) // math.isqrt(grade ** slope) + 1 for grade in range(1, number_of + 1)]
    largest = reach if full else min(reach, max(-(-total // number_of), total * weights[0] // sum(weights)))
    least = 1 if total - largest >= number_of - 1 else 0
    given, spare = [largest] + [least] * (number_of - 1), total - largest - least * (number_of - 1)
    while spare > 0:
        free = [i for i in range(1, number_of) if given[i] < largest] or [i for i in range(1, number_of) if given[i] < reach]
        pool, budget = sum([weights[i] for i in free]), spare
        for i in free:
            extra = min(reach - given[i], max(1, budget * weights[i] // pool), spare)
            given[i] = given[i] + extra
            spare = spare - extra
    return np.array(given)


def noise(key, shape, scale, most, split=(), kind=jnp.bfloat16):
    drawn = scale * jax.random.normal(key, shape, jnp.float32)
    if split:
        drawn = drawn * level_of(key, shape, split, -0.22, 0.18)
    return jnp.clip(drawn, -most, most).astype(kind)


def setup_inputs(seed: int = 0) -> dict:
    key_of = jax.random.split(jax.random.key(seed), 15)
    hidden = noise(key_of[0], (TOKENS, MODEL_WIDTH), 1.0, 6.0, ((0, 16), (1, 2)))
    routes_keys = jax.random.split(jax.random.fold_in(key_of[1], 1), TOKENS // T_DEV)
    routes_turns = jax.random.permutation(jax.random.fold_in(key_of[1], 3), TOKENS // T_DEV)
    routes = jax.vmap(lambda own, number: routed_block(jax.random.fold_in(key_of[1], 2), own, number, T_DEV, EXPERTS, TOP, CAP, 2))(routes_keys, routes_turns).reshape((TOKENS, TOP))
    routing_weights = jnp.clip(jnp.exp(math.log(1.0) - 2.9957323 * jax.random.uniform(key_of[2], (TOKENS, TOP), jnp.float32) ** level_of(key_of[2], (TOKENS, TOP), ((0, 16),), -0.2, 0.2)), 0.05, 1.0)
    w_gate = noise(key_of[3], (EXPERTS, MODEL_WIDTH, FF), MODEL_WIDTH ** -0.5, 0.09375, ((0, 16), (2, 2)))
    w_up = noise(key_of[4], (EXPERTS, MODEL_WIDTH, FF), MODEL_WIDTH ** -0.5, 0.09375, ((0, 16), (2, 2)))
    w_down = noise(key_of[5], (EXPERTS, FF, MODEL_WIDTH), FF ** -0.5, 0.15625, ((0, 16), (1, 2)))
    norm_gain = jnp.clip(1.0 + 0.18 * jax.random.normal(key_of[6], (MODEL_WIDTH,), jnp.float32), 0.1, 1.9)
    key_projection_weight = noise(key_of[7], (MODEL_WIDTH, KEY_VALUE_HEADS * HEAD_SIZE), MODEL_WIDTH ** -0.5, 0.09375, ((1, 2),))
    value_projection_weight = noise(key_of[8], (MODEL_WIDTH, KEY_VALUE_HEADS * HEAD_SIZE), MODEL_WIDTH ** -0.5, 0.09375, ((1, 2),))
    queries = draw_queries(jax.random.fold_in(key_of[14], 71), 0)
    cached_key_rows = draw_cached_key_rows(jax.random.fold_in(key_of[14], 71), 0)
    cached_value_rows = noise(key_of[11], (REQUEST_TOTAL, CONTEXT_SLOTS, KEY_VALUE_HEADS * HEAD_SIZE), 1.0, 6.0, ((0, 16), (2, 2)))
    lengths = set_ends(jax.random.randint(key_of[12], (REQUEST_TOTAL,), max(2, CONTEXT_SLOTS // 8), CONTEXT_SLOTS + 1), jax.random.fold_in(key_of[12], 1), max(2, CONTEXT_SLOTS // 8), CONTEXT_SLOTS).astype(jnp.int32)
    parents = draw_parents(jax.random.fold_in(key_of[14], 71), 0)
    return {"hidden": hidden, "routes": routes, "routing_weights": routing_weights, "w_gate": w_gate, "w_up": w_up, "w_down": w_down, "norm_gain": norm_gain, "key_projection_weight": key_projection_weight, "value_projection_weight": value_projection_weight, "queries": queries, "cached_key_rows": cached_key_rows, "cached_value_rows": cached_value_rows, "lengths": lengths, "parents": parents}


def ancestry(parent_row):
    node_count = parent_row.shape[0]
    position = jnp.arange(node_count, dtype=jnp.int32)
    reached = (parent_row[:, None] == position[None, :]).astype(jnp.float32)
    reached = reached + jnp.eye(node_count, dtype=jnp.float32)
    for doubling in range((node_count - 1).bit_length()):
        reached = jnp.minimum(jnp.dot(reached, reached, preferred_element_type=jnp.float32), 1.0)
    return reached > 0.5

def request_attention(inputs):
    request_query_rows, request_key_cache, request_value_cache, tree_key_rows, tree_value_rows, length, parent_row = inputs
    query_group_count = QUERY_HEADS // KEY_VALUE_HEADS
    scaled = 1.0 / math.sqrt(HEAD_SIZE)
    highest_precision = lax.Precision.HIGHEST
    tree_query_block = request_query_rows.astype(jnp.float32).reshape(TREE_TOKENS, KEY_VALUE_HEADS, query_group_count, HEAD_SIZE)
    joined_key_block = request_key_cache.astype(jnp.float32).reshape(CONTEXT_SLOTS, KEY_VALUE_HEADS, HEAD_SIZE)
    joined_value_block = request_value_cache.astype(jnp.float32).reshape(CONTEXT_SLOTS, KEY_VALUE_HEADS, HEAD_SIZE)
    tree_key_block = tree_key_rows.astype(jnp.float32).reshape(TREE_TOKENS, KEY_VALUE_HEADS, HEAD_SIZE)
    tree_value_block = tree_value_rows.astype(jnp.float32).reshape(TREE_TOKENS, KEY_VALUE_HEADS, HEAD_SIZE)
    cache_scores = jnp.einsum('nkgd,pkd->kgnp', tree_query_block, joined_key_block, precision=highest_precision) * scaled
    tree_scores = jnp.einsum('nkgd,mkd->kgnm', tree_query_block, tree_key_block, precision=highest_precision) * scaled
    visible = jnp.arange(CONTEXT_SLOTS, dtype=jnp.int32) < length
    cache_scores = jnp.where(visible[None, None, None, :], cache_scores, -1e+30)
    tree_scores = jnp.where(ancestry(parent_row)[None, None], tree_scores, -1e+30)
    scores = jnp.concatenate([cache_scores, tree_scores], axis=-1)
    highest = lax.optimization_barrier(jnp.max(scores, axis=-1, keepdims=True))
    raised = jnp.exp(scores - highest)
    soft_weights = (raised / lax.optimization_barrier(jnp.sum(raised, axis=-1, keepdims=True))).astype(jnp.bfloat16)
    soft_weights = lax.optimization_barrier(soft_weights).astype(jnp.float32)
    output = jnp.einsum('kgnp,pkd->nkgd', soft_weights[..., :CONTEXT_SLOTS], joined_value_block, precision=highest_precision)
    output = output + jnp.einsum('kgnm,mkd->nkgd', soft_weights[..., CONTEXT_SLOTS:], tree_value_block, precision=highest_precision)
    return output.reshape(TREE_TOKENS, QUERY_HEADS * HEAD_SIZE).astype(jnp.bfloat16)

def reference(hidden, routes, routing_weights, w_gate, w_up, w_down, norm_gain, key_projection_weight, value_projection_weight, queries, cached_key_rows, cached_value_rows, lengths, parents):
    weights = routing_weights / lax.optimization_barrier(jnp.sum(routing_weights, axis=1, keepdims=True))
    slot_total = N_DP * CAP
    padded = jnp.concatenate([hidden, jnp.zeros((1, MODEL_WIDTH), hidden.dtype)], axis=0)

    def one_expert(carried, expert):
        chosen = routes == expert
        picked = jnp.any(chosen, axis=1)
        portion = lax.optimization_barrier(jnp.sum(jnp.where(chosen, weights, 0.0), axis=1))
        members = jnp.nonzero(picked, size=slot_total, fill_value=TOKENS)[0].astype(jnp.int32)
        rows_in = jnp.take(padded, members, axis=0)
        gate_act = jnp.dot(rows_in, w_gate[expert], preferred_element_type=jnp.float32)
        upward = jnp.dot(rows_in, w_up[expert], preferred_element_type=jnp.float32)
        active = (jax.nn.silu(gate_act) * upward).astype(jnp.bfloat16)
        active = lax.optimization_barrier(active)
        pieces = active.astype(jnp.float32).reshape(slot_total, N_TP, FF // N_TP)
        down_rows = w_down[expert].astype(jnp.float32).reshape(N_TP, FF // N_TP, MODEL_WIDTH)
        partial_value = jnp.einsum('snf,nfd->nsd', pieces, down_rows, precision=lax.Precision.HIGHEST).astype(jnp.bfloat16)
        partial_value = lax.optimization_barrier(partial_value)
        summed = lax.optimization_barrier(jnp.sum(partial_value.astype(jnp.float32), axis=0))
        factor = jnp.take(jnp.concatenate([portion, jnp.zeros((1,), portion.dtype)]), members)
        carried = carried.at[members].add(factor[:, None] * summed, mode='drop')
        return (carried, None)
    expert_mix, unused = lax.scan(one_expert, jnp.zeros((TOKENS, MODEL_WIDTH), jnp.float32), jnp.arange(EXPERTS, dtype=jnp.int32))
    layer_output = (hidden.astype(jnp.float32) + expert_mix).astype(jnp.bfloat16)
    widened = layer_output.astype(jnp.float32)
    scaling = lax.rsqrt(lax.optimization_barrier(jnp.mean(widened * widened, axis=1, keepdims=True)) + 1e-06)
    normed = (widened * scaling * norm_gain).astype(jnp.bfloat16)
    next_layer_keys = jnp.dot(normed, key_projection_weight, preferred_element_type=jnp.float32).astype(jnp.bfloat16)
    next_layer_values = jnp.dot(normed, value_projection_weight, preferred_element_type=jnp.float32).astype(jnp.bfloat16)
    attended = lax.map(request_attention, (queries.reshape(REQUEST_TOTAL, TREE_TOKENS, QUERY_HEADS * HEAD_SIZE), cached_key_rows, cached_value_rows, next_layer_keys.reshape(REQUEST_TOTAL, TREE_TOKENS, KEY_VALUE_HEADS * HEAD_SIZE), next_layer_values.reshape(REQUEST_TOTAL, TREE_TOKENS, KEY_VALUE_HEADS * HEAD_SIZE), lengths, parents))
    return (layer_output, next_layer_keys, next_layer_values, attended.reshape(TOKENS, QUERY_HEADS * HEAD_SIZE))
```

```python
import math

import functools

import jax
import jax.numpy as jnp
from jax import lax
from jax.experimental import pallas as pl
from jax.experimental.pallas import tpu as pltpu
from jax.sharding import PartitionSpec as P

HEAD_SIZE = 128


def ancestry(parent_row):
    node_count = parent_row.shape[0]
    position = jnp.arange(node_count, dtype=jnp.int32)
    reached = (parent_row[:, None] == position[None, :]).astype(jnp.float32)
    reached = reached + jnp.eye(node_count, dtype=jnp.float32)
    for doubling in range((node_count - 1).bit_length()):
        reached = jnp.minimum(jnp.dot(reached, reached, preferred_element_type=jnp.float32), 1.0)
    return reached > 0.5

CORES = 2
COLUMNS = 2
PIECES = 8


def expert_kernel(
    planes,
    hidden_ref,
    share_ref,
    gate_ref,
    up_ref,
    down_ref,
    own_ref,
    full_ref,
    rows,
    shares,
    gate,
    up,
    down,
    gate_total,
    up_total,
    active,
    factor,
    mixed,
    from_core,
    from_first,
    from_second,
    from_plane,
    whole,
    local_sems,
    send_sems,
    recv_sems,
):
    me = lax.axis_index("dp")
    side = lax.axis_index("tp")
    core = lax.rem(me, CORES)
    column = lax.rem(me // CORES, COLUMNS)
    plane = me // (CORES * COLUMNS)
    pieces = rows.shape[0]
    width = rows.shape[-1]
    row_count = rows.shape[2] * rows.shape[3] * rows.shape[4] * rows.shape[5]
    half = pieces * width
    ff = gate.shape[-1]

    def device(plane_, column_, core_, side_):
        return ((plane_ * COLUMNS + column_) * CORES + core_, side_)

    over_core = device(plane, column, 1 - core, side)
    over_column = device(plane, 1 - column, core, side)
    over_side = device(plane, column, core, 1 - side)
    others = [lax.rem(plane + k, planes) for k in range(1, planes)]
    over_planes = [device(o, column, core, side) for o in others]

    local_count = [0]

    def local(source, target):
        copy = pltpu.make_async_copy(source, target, local_sems.at[local_count[0]])
        local_count[0] += 1
        copy.start()
        return copy

    own_loads = [
        local(
            hidden_ref.at[:, pl.ds(p * width, width)], rows.at[p, side, core, column, plane]
        )
        for p in range(pieces)
    ]
    share_load = local(share_ref, shares.at[core, column, plane])

    barrier = pltpu.get_barrier_semaphore()
    partners = over_planes + [over_column, over_side, over_core]
    for partner in partners:
        pl.semaphore_signal(
            barrier, inc=1, device_id=partner, device_id_type=pl.DeviceIdType.MESH
        )
    for copy in own_loads:
        copy.wait()
    share_load.wait()
    pl.semaphore_wait(barrier, len(partners))

    remote_count = [0]
    sent = []

    def remote(source, target, where):
        index = remote_count[0]
        remote_count[0] += 1
        copy = pltpu.make_async_remote_copy(
            src_ref=source,
            dst_ref=target,
            send_sem=send_sems.at[index],
            recv_sem=recv_sems.at[index],
            device_id=where,
            device_id_type=pl.DeviceIdType.MESH,
        )
        copy.start()
        sent.append(copy)
        return copy

    share_slot = shares.at[core, column, plane]
    by_plane = {}
    for p in range(pieces):
        slot = rows.at[p, side, core, column, plane]
        by_plane[p] = [remote(slot, slot, where) for where in over_planes]
        if p == 0:
            share_moves = [remote(share_slot, share_slot, where) for where in over_planes]

    gate_loads, up_loads = [], []
    for p in range(pieces):
        gate_loads.append(local(gate_ref.at[:, p], gate.at[:, p]))
        up_loads.append(local(up_ref.at[:, p], up.at[:, p]))
    down_load = local(down_ref, down)

    first, second, across = {}, {}, {}
    tile = 256 if ff % 256 == 0 else ff

    def multiply(p):
        gate_loads[p].wait()
        up_loads[p].wait()

        def one(n, carry):
            columns = pl.ds(pl.multiple_of(n * tile, tile), tile)
            for weight, total in ((gate, gate_total), (up, up_total)):
                added = None
                for s in range(2):
                    term = jnp.dot(
                        rows[p, s].reshape(row_count, width),
                        weight[s, p, :, columns],
                        preferred_element_type=jnp.float32,
                    )
                    added = term if added is None else added + term
                if p > 0:
                    added = added + total[:, columns]
                total[:, columns] = added
            return carry

        lax.fori_loop(0, ff // tile, one, 0)

    for step in range(pieces + 3):
        p = step
        if p < pieces:
            for copy in by_plane[p]:
                copy.wait_recv()
            block = rows.at[p, side, core, column]
            first[p] = remote(block, block, over_column if p % 2 == 0 else over_side)
            if p == 0:
                for copy in share_moves:
                    copy.wait_recv()
                share_block = shares.at[core, column]
                share_first = remote(share_block, share_block, over_column)
        p = step - 1
        if 0 <= p < pieces:
            first[p].wait_recv()
            if p % 2 == 0:
                block = rows.at[p, side, core]
                second[p] = remote(block, block, over_side)
            else:
                block = rows.at[p, :, core, column]
                second[p] = remote(block, block, over_column)
            if p == 0:
                share_first.wait_recv()
                share_across = remote(shares.at[core], shares.at[core], over_core)
        p = step - 2
        if 0 <= p < pieces:
            second[p].wait_recv()
            block = rows.at[p, :, core]
            across[p] = remote(block, block, over_core)
        p = step - 3
        if 0 <= p < pieces:
            across[p].wait_recv()
            if p == 0:
                share_across.wait_recv()
                tokens, lanes = rows.shape[5], factor.shape[1]
                diagonal = lax.broadcasted_iota(
                    jnp.int32, (tokens, lanes), 0
                ) == lax.broadcasted_iota(jnp.int32, (tokens, lanes), 1)
                place = 0
                for c in range(CORES):
                    for x in range(COLUMNS):
                        for z in range(planes):
                            row = shares[c, x, z, pl.ds(me, 1), :]
                            value = jnp.sum(
                                jnp.where(diagonal, row, 0.0), axis=1, keepdims=True
                            )
                            factor[pl.ds(place * tokens, tokens), :] = jnp.broadcast_to(
                                value, (tokens, lanes)
                            )
                            place += 1
            multiply(p)

    lanes = factor.shape[1]

    def activate(n, carry):
        columns = pl.ds(pl.multiple_of(n * lanes, lanes), lanes)
        value = gate_total[:, columns]
        value = value / (1.0 + jnp.exp(-value)) * up_total[:, columns] * factor[...]
        active[:, columns] = value.astype(active.dtype)
        return carry

    lax.fori_loop(0, ff // lanes, activate, 0)
    down_load.wait()

    core_moves, first_moves, second_moves, plane_moves, side_moves = {}, {}, {}, {}, {}

    def project(p):
        def one(s, carry):
            columns = pl.ds(pl.multiple_of(s * half + p * width, width), width)
            value = jnp.dot(active[...], down[:, columns], preferred_element_type=jnp.float32)
            mixed[p, s] = value.astype(mixed.dtype).reshape(mixed.shape[2:])
            return carry

        lax.fori_loop(0, 2, one, 0)
        core_moves[p] = remote(mixed.at[p, :, 1 - core], from_core.at[p], over_core)

    def add(target, other):
        target[...] = (
            target[...].astype(jnp.float32) + other[...].astype(jnp.float32)
        ).astype(target.dtype)

    for step in range(pieces + 5):
        p = step
        if p < pieces:
            project(p)
        p = step - 1
        if 0 <= p < pieces:
            core_moves[p].wait_recv()
            add(mixed.at[p, :, core], from_core.at[p])
            landing = from_first.at[p]
            if p % 2 == 0:
                first_moves[p] = remote(mixed.at[p, 1 - side, core], landing, over_side)
            else:
                first_moves[p] = remote(mixed.at[p, :, core, 1 - column], landing, over_column)
        p = step - 2
        if 0 <= p < pieces:
            first_moves[p].wait_recv()
            landing = from_second.at[p]
            if p % 2 == 0:
                add(mixed.at[p, side, core], from_first.at[p])
                second_moves[p] = remote(
                    mixed.at[p, side, core, 1 - column], landing, over_column
                )
            else:
                add(mixed.at[p, :, core, column], from_first.at[p])
                second_moves[p] = remote(
                    mixed.at[p, 1 - side, core, column], landing, over_side
                )
        p = step - 3
        if 0 <= p < pieces:
            second_moves[p].wait_recv()
            add(mixed.at[p, side, core, column], from_second.at[p])
            plane_moves[p] = [
                remote(mixed.at[p, side, core, column, o], from_plane.at[p, k], where)
                for k, (o, where) in enumerate(zip(others, over_planes))
            ]
        p = step - 4
        if 0 <= p < pieces:
            total = mixed[p, side, core, column, plane].astype(jnp.float32)
            for k, copy in enumerate(plane_moves[p]):
                copy.wait_recv()
                total = total + from_plane[p, k].astype(jnp.float32)
            total = total + rows[p, side, core, column, plane].astype(jnp.float32)
            total = total.astype(own_ref.dtype)
            own_ref[:, pl.ds(p * width, width)] = total
            whole[side, p] = total
            side_moves[p] = remote(whole.at[side, p], whole.at[side, p], over_side)

    for p in range(pieces):
        side_moves[p].wait_recv()
        for s in range(2):
            full_ref[:, pl.ds(s * half + p * width, width)] = whole[s, p]
    for copy in sent:
        copy.wait_send()


def dense_experts(hidden, shares, w_gate, w_up, w_down):
    token_count, half = hidden.shape
    expert_count = shares.shape[0]
    planes = lax.axis_size("dp") // (CORES * COLUMNS)
    ff = w_gate.shape[2]
    pieces = PIECES
    width = half // pieces
    model_width = w_gate.shape[1]
    gate = w_gate.reshape(2, pieces, width, ff)
    up = w_up.reshape(2, pieces, width, ff)
    down = w_down.reshape(ff, model_width)
    lanes = shares.shape[1]
    row_count = CORES * COLUMNS * planes * token_count
    bf, f32 = jnp.bfloat16, jnp.float32
    blocks = (token_count, width)
    copies = pieces * (2 * (planes - 1) + 7) + planes + 1
    anywhere = pl.BlockSpec(memory_space=pl.ANY)
    inside = pl.BlockSpec(memory_space=pltpu.VMEM)
    return pl.pallas_call(
        functools.partial(expert_kernel, planes),
        out_shape=(
            jax.ShapeDtypeStruct((token_count, half), bf),
            jax.ShapeDtypeStruct((token_count, 2 * half), bf),
        ),
        in_specs=[anywhere] * 5,
        out_specs=(inside, inside),
        scratch_shapes=[
            pltpu.VMEM((pieces, 2, CORES, COLUMNS, planes, *blocks), bf),
            pltpu.VMEM((CORES, COLUMNS, planes, expert_count, lanes), f32),
            pltpu.VMEM((2, pieces, width, ff), bf),
            pltpu.VMEM((2, pieces, width, ff), bf),
            pltpu.VMEM((ff, model_width), bf),
            pltpu.VMEM((row_count, ff), f32),
            pltpu.VMEM((row_count, ff), f32),
            pltpu.VMEM((row_count, ff), bf),
            pltpu.VMEM((row_count, lanes), f32),
            pltpu.VMEM((pieces, 2, CORES, COLUMNS, planes, *blocks), bf),
            pltpu.VMEM((pieces, 2, COLUMNS, planes, *blocks), bf),
            pltpu.VMEM((pieces, 2, planes, *blocks), bf),
            pltpu.VMEM((pieces, planes, *blocks), bf),
            pltpu.VMEM((pieces, planes - 1, *blocks), bf),
            pltpu.VMEM((2, pieces, *blocks), bf),
            pltpu.SemaphoreType.DMA((3 * pieces + 2,)),
            pltpu.SemaphoreType.DMA((copies,)),
            pltpu.SemaphoreType.DMA((copies,)),
        ],
        compiler_params=pltpu.CompilerParams(
            collective_id=0, has_side_effects=True, vmem_limit_bytes=60 * 1024 * 1024
        ),
        name="dense_experts",
    )(hidden, shares, gate, up, down)


def full_rows(hidden):
    return lax.all_gather(hidden, "tp", axis=1, tiled=True)


def attend_local(
    queries, cached_key_rows, cached_value_rows, tree_key_rows, tree_value_rows, lengths, parents
):
    request_count = lengths.shape[0]
    node_count = parents.shape[1]
    slot_length = cached_key_rows.shape[1]
    kv_local = cached_key_rows.shape[2] // HEAD_SIZE
    query_group_count = queries.shape[1] // (kv_local * HEAD_SIZE)
    scaled = 1.0 / math.sqrt(HEAD_SIZE)
    tree_query_block = queries.reshape(
        request_count, node_count, kv_local, query_group_count, HEAD_SIZE
    )
    joined_key_block = cached_key_rows.reshape(request_count, slot_length, kv_local, HEAD_SIZE)
    joined_value_block = cached_value_rows.reshape(request_count, slot_length, kv_local, HEAD_SIZE)
    tree_key_block = tree_key_rows.reshape(request_count, node_count, kv_local, HEAD_SIZE)
    tree_value_block = tree_value_rows.reshape(request_count, node_count, kv_local, HEAD_SIZE)
    cache_scores = (
        jnp.einsum(
            "rnkgd,rpkd->rkgnp",
            tree_query_block,
            joined_key_block,
            preferred_element_type=jnp.float32,
        )
        * scaled
    )
    tree_scores = (
        jnp.einsum(
            "rnkgd,rmkd->rkgnm",
            tree_query_block,
            tree_key_block,
            preferred_element_type=jnp.float32,
        )
        * scaled
    )
    visible = jnp.arange(slot_length, dtype=jnp.int32)[None, :] < lengths[:, None]
    cache_scores = jnp.where(visible[:, None, None, None, :], cache_scores, -1e30)
    related = jax.vmap(ancestry)(parents)
    tree_scores = jnp.where(related[:, None, None], tree_scores, -1e30)
    highest = jnp.maximum(jnp.max(cache_scores, axis=-1), jnp.max(tree_scores, axis=-1))[..., None]
    cache_raised = jnp.exp(cache_scores - highest)
    tree_raised = jnp.exp(tree_scores - highest)
    denominator = jnp.sum(cache_raised, axis=-1, keepdims=True) + jnp.sum(
        tree_raised, axis=-1, keepdims=True
    )
    cache_weights = (cache_raised / denominator).astype(jnp.bfloat16)
    tree_weights = (tree_raised / denominator).astype(jnp.bfloat16)
    output = jnp.einsum(
        "rkgnp,rpkd->rnkgd", cache_weights, joined_value_block, preferred_element_type=jnp.float32
    )
    output = output + jnp.einsum(
        "rkgnm,rmkd->rnkgd", tree_weights, tree_value_block, preferred_element_type=jnp.float32
    )
    return output.reshape(request_count * node_count, -1).astype(jnp.bfloat16)


LANES = 128


def dense_fits(hidden, routes, w_gate):
    token_count, half = hidden.shape
    expert_count = lax.axis_size("dp") * w_gate.shape[0]
    return (
        2 * token_count * routes.shape[1] // expert_count >= token_count
        and w_gate.shape[0] == 1
        and lax.axis_size("tp") == 2
        and lax.axis_size("dp") % (CORES * COLUMNS) == 0
        and lax.axis_size("dp") > CORES * COLUMNS
        and token_count % 16 == 0
        and token_count <= LANES
        and half % (PIECES * LANES) == 0
        and w_gate.shape[2] % LANES == 0
    )


def routed_experts(hidden, routes, weights, w_gate, w_up, w_down):
    token_count = hidden.shape[0]
    top_count = routes.shape[1]
    local_experts = w_gate.shape[0]
    expert_count = lax.axis_size("dp") * local_experts
    capacity = min(token_count, 2 * token_count * top_count // expert_count)
    flat_routes = routes.reshape(-1)
    expert_ids = jnp.arange(expert_count, dtype=jnp.int32)
    matches = (flat_routes[:, None] == expert_ids[None, :]).astype(jnp.int32)
    running = jnp.cumsum(matches, axis=0)
    slot_index = jnp.sum(matches * running, axis=1) - 1
    targets = flat_routes * capacity + slot_index
    owners = jnp.arange(token_count * top_count, dtype=jnp.int32) // top_count
    token_table = (
        jnp.full((expert_count * capacity,), token_count, jnp.int32).at[targets].set(owners)
    )
    whole_rows = None
    whole_rows = full_rows(hidden)
    padded = jnp.concatenate(
        [whole_rows, jnp.zeros((1, whole_rows.shape[1]), whole_rows.dtype)], axis=0
    )
    outgoing = jnp.take(padded, token_table, axis=0).reshape(
        expert_count, capacity, whole_rows.shape[1]
    )
    received = lax.all_to_all(outgoing, "dp", split_axis=0, concat_axis=0, tiled=True)
    slot_count = received.shape[1]
    grouped = received.reshape(-1, local_experts, slot_count, received.shape[2])
    gate_act = jnp.einsum("secd,edf->secf", grouped, w_gate, preferred_element_type=jnp.float32)
    upward = jnp.einsum("secd,edf->secf", grouped, w_up, preferred_element_type=jnp.float32)
    active = (jax.nn.silu(gate_act) * upward).astype(jnp.bfloat16)
    partial_value = jnp.einsum("secf,efd->secd", active, w_down, preferred_element_type=jnp.float32)
    partial_value = partial_value.reshape(received.shape[0], slot_count, partial_value.shape[3])
    summed = lax.psum_scatter(
        partial_value.astype(jnp.bfloat16), "tp", scatter_dimension=2, tiled=True
    ).astype(jnp.float32)
    back = lax.all_to_all(
        summed.astype(jnp.bfloat16), "dp", split_axis=0, concat_axis=0, tiled=True
    ).astype(summed.dtype)
    flat_back = back.reshape(expert_count * capacity, back.shape[2])
    picked = jnp.take(flat_back, targets, axis=0).reshape(token_count, top_count, back.shape[2])
    expert_mix = jnp.sum(weights[:, :, None] * picked, axis=1)
    own_out = (hidden.astype(jnp.float32) + expert_mix).astype(jnp.bfloat16)
    full_out = lax.all_gather(own_out, "tp", axis=1, tiled=True)
    return own_out, full_out


def on_device(
    hidden,
    routes,
    routing_weights,
    w_gate,
    w_up,
    w_down,
    norm_gain,
    key_projection_weight,
    value_projection_weight,
    queries,
    cached_key_rows,
    cached_value_rows,
    lengths,
    parents,
):
    token_count = hidden.shape[0]
    expert_count = lax.axis_size("dp") * w_gate.shape[0]
    weights = routing_weights / jnp.sum(routing_weights, axis=1, keepdims=True)
    if dense_fits(hidden, routes, w_gate):
        expert_ids = jnp.arange(expert_count, dtype=jnp.int32)
        named = routes.T[None, :, :] == expert_ids[:, None, None]
        shares = jnp.sum(jnp.where(named, weights.T[None, :, :], 0.0), axis=1)
        shares = jnp.pad(shares, ((0, 0), (0, LANES - token_count)))
        own_out, full_out = dense_experts(hidden, shares, w_gate, w_up, w_down)
    else:
        own_out, full_out = routed_experts(
            hidden, routes, weights, w_gate, w_up, w_down
        )
    widened = full_out.astype(jnp.float32)
    scaling = lax.rsqrt(jnp.mean(widened * widened, axis=1, keepdims=True) + 1e-06)
    normed = (widened * scaling * norm_gain).astype(jnp.bfloat16)
    tree_key_rows = jnp.dot(
        normed, key_projection_weight, preferred_element_type=jnp.float32
    ).astype(jnp.bfloat16)
    tree_value_rows = jnp.dot(
        normed, value_projection_weight, preferred_element_type=jnp.float32
    ).astype(jnp.bfloat16)
    attended = attend_local(
        queries,
        cached_key_rows,
        cached_value_rows,
        tree_key_rows,
        tree_value_rows,
        lengths,
        parents,
    )
    return (own_out, tree_key_rows, tree_value_rows, attended)


def solution(mesh):
    return jax.shard_map(
        on_device,
        mesh=mesh,
        in_specs=(
            P("dp", "tp"),
            P("dp", None),
            P("dp", None),
            P("dp", None, "tp"),
            P("dp", None, "tp"),
            P("dp", "tp", None),
            P(),
            P(None, "tp"),
            P(None, "tp"),
            P("dp", "tp"),
            P("dp", None, "tp"),
            P("dp", None, "tp"),
            P("dp"),
            P("dp", None),
        ),
        out_specs=(P("dp", "tp"), P("dp", "tp"), P("dp", "tp"), P("dp", "tp")),
        check_vma=False,
    )
```

```python
import math

import functools

import jax
import jax.numpy as jnp
from jax import lax
from jax.experimental import pallas as pl
from jax.experimental.pallas import tpu as pltpu
from jax.sharding import PartitionSpec as P

HEAD_SIZE = 128


def ancestry(parent_row):
    node_count = parent_row.shape[0]
    position = jnp.arange(node_count, dtype=jnp.int32)
    reached = (parent_row[:, None] == position[None, :]).astype(jnp.float32)
    reached = reached + jnp.eye(node_count, dtype=jnp.float32)
    for doubling in range((node_count - 1).bit_length()):
        reached = jnp.minimum(jnp.dot(reached, reached, preferred_element_type=jnp.float32), 1.0)
    return reached > 0.5

CORES = 2
COLUMNS = 2
PIECES = 8


def expert_kernel(
    planes,
    hidden_ref,
    share_ref,
    gate_ref,
    up_ref,
    down_ref,
    own_ref,
    full_ref,
    rows,
    shares,
    gate,
    up,
    down,
    gate_total,
    up_total,
    active,
    factor,
    mixed,
    from_core,
    from_first,
    from_second,
    from_plane,
    whole,
    local_sems,
    send_sems,
    recv_sems,
):
    me = lax.axis_index("dp")
    side = lax.axis_index("tp")
    core = lax.rem(me, CORES)
    column = lax.rem(me // CORES, COLUMNS)
    plane = me // (CORES * COLUMNS)
    pieces = rows.shape[0]
    width = rows.shape[-1]
    row_count = rows.shape[2] * rows.shape[3] * rows.shape[4] * rows.shape[5]
    half = pieces * width
    ff = gate.shape[-1]

    def device(plane_, column_, core_, side_):
        return ((plane_ * COLUMNS + column_) * CORES + core_, side_)

    over_core = device(plane, column, 1 - core, side)
    over_column = device(plane, 1 - column, core, side)
    over_side = device(plane, column, core, 1 - side)
    others = [lax.rem(plane + k, planes) for k in range(1, planes)]
    over_planes = [device(o, column, core, side) for o in others]

    local_count = [0]

    def local(source, target):
        copy = pltpu.make_async_copy(source, target, local_sems.at[local_count[0]])
        local_count[0] += 1
        copy.start()
        return copy

    own_loads = [
        local(
            hidden_ref.at[:, pl.ds(p * width, width)], rows.at[p, side, core, column, plane]
        )
        for p in range(pieces)
    ]
    share_load = local(share_ref, shares.at[core, column, plane])

    barrier = pltpu.get_barrier_semaphore()
    partners = over_planes + [over_column, over_side, over_core]
    for partner in partners:
        pl.semaphore_signal(
            barrier, inc=1, device_id=partner, device_id_type=pl.DeviceIdType.MESH
        )
    for copy in own_loads:
        copy.wait()
    share_load.wait()
    pl.semaphore_wait(barrier, len(partners))

    remote_count = [0]
    sent = []

    def remote(source, target, where):
        index = remote_count[0]
        remote_count[0] += 1
        copy = pltpu.make_async_remote_copy(
            src_ref=source,
            dst_ref=target,
            send_sem=send_sems.at[index],
            recv_sem=recv_sems.at[index],
            device_id=where,
            device_id_type=pl.DeviceIdType.MESH,
        )
        copy.start()
        sent.append(copy)
        return copy

    share_slot = shares.at[core, column, plane]
    by_plane = {}
    for p in range(pieces):
        slot = rows.at[p, side, core, column, plane]
        by_plane[p] = [remote(slot, slot, where) for where in over_planes]
        if p == 0:
            share_moves = [remote(share_slot, share_slot, where) for where in over_planes]

    gate_loads, up_loads = [], []
    for p in range(pieces):
        gate_loads.append(local(gate_ref.at[:, p], gate.at[:, p]))
        up_loads.append(local(up_ref.at[:, p], up.at[:, p]))
    down_load = local(down_ref, down)

    first, second, across = {}, {}, {}
    tile = 256 if ff % 256 == 0 else ff

    def multiply(p):
        gate_loads[p].wait()
        up_loads[p].wait()

        def one(n, carry):
            columns = pl.ds(pl.multiple_of(n * tile, tile), tile)
            for weight, total in ((gate, gate_total), (up, up_total)):
                added = None
                for s in range(2):
                    term = jnp.dot(
                        rows[p, s].reshape(row_count, width),
                        weight[s, p, :, columns],
                        preferred_element_type=jnp.float32,
                    )
                    added = term if added is None else added + term
                if p > 0:
                    added = added + total[:, columns]
                total[:, columns] = added
            return carry

        lax.fori_loop(0, ff // tile, one, 0)

    for step in range(pieces + 5):
        p = step
        if p < pieces:
            for copy in by_plane[p]:
                copy.wait_recv()
            block = rows.at[p, side, core, column]
            first[p] = remote(block, block, over_column if p % 2 == 0 else over_side)
            if p == 0:
                for copy in share_moves:
                    copy.wait_recv()
                share_block = shares.at[core, column]
                share_first = remote(share_block, share_block, over_column)
        p = step - 2
        if 0 <= p < pieces:
            first[p].wait_recv()
            if p % 2 == 0:
                block = rows.at[p, side, core]
                second[p] = remote(block, block, over_side)
            else:
                block = rows.at[p, :, core, column]
                second[p] = remote(block, block, over_column)
            if p == 0:
                share_first.wait_recv()
                share_across = remote(shares.at[core], shares.at[core], over_core)
        p = step - 4
        if 0 <= p < pieces:
            second[p].wait_recv()
            block = rows.at[p, :, core]
            across[p] = remote(block, block, over_core)
        p = step - 5
        if 0 <= p < pieces:
            across[p].wait_recv()
            if p == 0:
                share_across.wait_recv()
                tokens, lanes = rows.shape[5], factor.shape[1]
                diagonal = lax.broadcasted_iota(
                    jnp.int32, (tokens, lanes), 0
                ) == lax.broadcasted_iota(jnp.int32, (tokens, lanes), 1)
                place = 0
                for c in range(CORES):
                    for x in range(COLUMNS):
                        for z in range(planes):
                            row = shares[c, x, z, pl.ds(me, 1), :]
                            value = jnp.sum(
                                jnp.where(diagonal, row, 0.0), axis=1, keepdims=True
                            )
                            factor[pl.ds(place * tokens, tokens), :] = jnp.broadcast_to(
                                value, (tokens, lanes)
                            )
                            place += 1
            multiply(p)

    lanes = factor.shape[1]

    def activate(n, carry):
        columns = pl.ds(pl.multiple_of(n * lanes, lanes), lanes)
        value = gate_total[:, columns]
        value = value / (1.0 + jnp.exp(-value)) * up_total[:, columns] * factor[...]
        active[:, columns] = value.astype(active.dtype)
        return carry

    lax.fori_loop(0, ff // lanes, activate, 0)
    down_load.wait()

    core_moves, first_moves, second_moves, plane_moves, side_moves = {}, {}, {}, {}, {}

    def project(p):
        def one(s, carry):
            columns = pl.ds(pl.multiple_of(s * half + p * width, width), width)
            value = jnp.dot(active[...], down[:, columns], preferred_element_type=jnp.float32)
            mixed[p, s] = value.astype(mixed.dtype).reshape(mixed.shape[2:])
            return carry

        lax.fori_loop(0, 2, one, 0)
        core_moves[p] = remote(mixed.at[p, :, 1 - core], from_core.at[p], over_core)

    def add(target, other):
        target[...] = (
            target[...].astype(jnp.float32) + other[...].astype(jnp.float32)
        ).astype(target.dtype)

    for step in range(pieces + 7):
        p = step
        if p < pieces:
            project(p)
        p = step - 1
        if 0 <= p < pieces:
            core_moves[p].wait_recv()
            add(mixed.at[p, :, core], from_core.at[p])
            landing = from_first.at[p]
            if p % 2 == 0:
                first_moves[p] = remote(mixed.at[p, 1 - side, core], landing, over_side)
            else:
                first_moves[p] = remote(mixed.at[p, :, core, 1 - column], landing, over_column)
        p = step - 3
        if 0 <= p < pieces:
            first_moves[p].wait_recv()
            landing = from_second.at[p]
            if p % 2 == 0:
                add(mixed.at[p, side, core], from_first.at[p])
                second_moves[p] = remote(
                    mixed.at[p, side, core, 1 - column], landing, over_column
                )
            else:
                add(mixed.at[p, :, core, column], from_first.at[p])
                second_moves[p] = remote(
                    mixed.at[p, 1 - side, core, column], landing, over_side
                )
        p = step - 5
        if 0 <= p < pieces:
            second_moves[p].wait_recv()
            add(mixed.at[p, side, core, column], from_second.at[p])
            plane_moves[p] = [
                remote(mixed.at[p, side, core, column, o], from_plane.at[p, k], where)
                for k, (o, where) in enumerate(zip(others, over_planes))
            ]
        p = step - 7
        if 0 <= p < pieces:
            total = mixed[p, side, core, column, plane].astype(jnp.float32)
            for k, copy in enumerate(plane_moves[p]):
                copy.wait_recv()
                total = total + from_plane[p, k].astype(jnp.float32)
            total = total + rows[p, side, core, column, plane].astype(jnp.float32)
            total = total.astype(own_ref.dtype)
            own_ref[:, pl.ds(p * width, width)] = total
            whole[side, p] = total
            side_moves[p] = remote(whole.at[side, p], whole.at[side, p], over_side)

    for p in range(pieces):
        side_moves[p].wait_recv()
        for s in range(2):
            full_ref[:, pl.ds(s * half + p * width, width)] = whole[s, p]
    for copy in sent:
        copy.wait_send()


def dense_experts(hidden, shares, w_gate, w_up, w_down):
    token_count, half = hidden.shape
    expert_count = shares.shape[0]
    planes = lax.axis_size("dp") // (CORES * COLUMNS)
    ff = w_gate.shape[2]
    pieces = PIECES
    width = half // pieces
    model_width = w_gate.shape[1]
    gate = w_gate.reshape(2, pieces, width, ff)
    up = w_up.reshape(2, pieces, width, ff)
    down = w_down.reshape(ff, model_width)
    lanes = shares.shape[1]
    row_count = CORES * COLUMNS * planes * token_count
    bf, f32 = jnp.bfloat16, jnp.float32
    blocks = (token_count, width)
    copies = pieces * (2 * (planes - 1) + 7) + planes + 1
    anywhere = pl.BlockSpec(memory_space=pl.ANY)
    inside = pl.BlockSpec(memory_space=pltpu.VMEM)
    return pl.pallas_call(
        functools.partial(expert_kernel, planes),
        out_shape=(
            jax.ShapeDtypeStruct((token_count, half), bf),
            jax.ShapeDtypeStruct((token_count, 2 * half), bf),
        ),
        in_specs=[anywhere] * 5,
        out_specs=(inside, inside),
        scratch_shapes=[
            pltpu.VMEM((pieces, 2, CORES, COLUMNS, planes, *blocks), bf),
            pltpu.VMEM((CORES, COLUMNS, planes, expert_count, lanes), f32),
            pltpu.VMEM((2, pieces, width, ff), bf),
            pltpu.VMEM((2, pieces, width, ff), bf),
            pltpu.VMEM((ff, model_width), bf),
            pltpu.VMEM((row_count, ff), f32),
            pltpu.VMEM((row_count, ff), f32),
            pltpu.VMEM((row_count, ff), bf),
            pltpu.VMEM((row_count, lanes), f32),
            pltpu.VMEM((pieces, 2, CORES, COLUMNS, planes, *blocks), bf),
            pltpu.VMEM((pieces, 2, COLUMNS, planes, *blocks), bf),
            pltpu.VMEM((pieces, 2, planes, *blocks), bf),
            pltpu.VMEM((pieces, planes, *blocks), bf),
            pltpu.VMEM((pieces, planes - 1, *blocks), bf),
            pltpu.VMEM((2, pieces, *blocks), bf),
            pltpu.SemaphoreType.DMA((3 * pieces + 2,)),
            pltpu.SemaphoreType.DMA((copies,)),
            pltpu.SemaphoreType.DMA((copies,)),
        ],
        compiler_params=pltpu.CompilerParams(
            collective_id=0, has_side_effects=True, vmem_limit_bytes=60 * 1024 * 1024
        ),
        name="dense_experts",
    )(hidden, shares, gate, up, down)


def full_rows(hidden):
    return lax.all_gather(hidden, "tp", axis=1, tiled=True)


def attend_local(
    queries, cached_key_rows, cached_value_rows, tree_key_rows, tree_value_rows, lengths, parents
):
    request_count = lengths.shape[0]
    node_count = parents.shape[1]
    slot_length = cached_key_rows.shape[1]
    kv_local = cached_key_rows.shape[2] // HEAD_SIZE
    query_group_count = queries.shape[1] // (kv_local * HEAD_SIZE)
    scaled = 1.0 / math.sqrt(HEAD_SIZE)
    tree_query_block = queries.reshape(
        request_count, node_count, kv_local, query_group_count, HEAD_SIZE
    )
    joined_key_block = cached_key_rows.reshape(request_count, slot_length, kv_local, HEAD_SIZE)
    joined_value_block = cached_value_rows.reshape(request_count, slot_length, kv_local, HEAD_SIZE)
    tree_key_block = tree_key_rows.reshape(request_count, node_count, kv_local, HEAD_SIZE)
    tree_value_block = tree_value_rows.reshape(request_count, node_count, kv_local, HEAD_SIZE)
    cache_scores = (
        jnp.einsum(
            "rnkgd,rpkd->rkgnp",
            tree_query_block,
            joined_key_block,
            preferred_element_type=jnp.float32,
        )
        * scaled
    )
    tree_scores = (
        jnp.einsum(
            "rnkgd,rmkd->rkgnm",
            tree_query_block,
            tree_key_block,
            preferred_element_type=jnp.float32,
        )
        * scaled
    )
    visible = jnp.arange(slot_length, dtype=jnp.int32)[None, :] < lengths[:, None]
    cache_scores = jnp.where(visible[:, None, None, None, :], cache_scores, -1e30)
    related = jax.vmap(ancestry)(parents)
    tree_scores = jnp.where(related[:, None, None], tree_scores, -1e30)
    highest = jnp.maximum(jnp.max(cache_scores, axis=-1), jnp.max(tree_scores, axis=-1))[..., None]
    cache_raised = jnp.exp(cache_scores - highest)
    tree_raised = jnp.exp(tree_scores - highest)
    denominator = jnp.sum(cache_raised, axis=-1, keepdims=True) + jnp.sum(
        tree_raised, axis=-1, keepdims=True
    )
    cache_weights = (cache_raised / denominator).astype(jnp.bfloat16)
    tree_weights = (tree_raised / denominator).astype(jnp.bfloat16)
    output = jnp.einsum(
        "rkgnp,rpkd->rnkgd", cache_weights, joined_value_block, preferred_element_type=jnp.float32
    )
    output = output + jnp.einsum(
        "rkgnm,rmkd->rnkgd", tree_weights, tree_value_block, preferred_element_type=jnp.float32
    )
    return output.reshape(request_count * node_count, -1).astype(jnp.bfloat16)


LANES = 128


def dense_fits(hidden, routes, w_gate):
    token_count, half = hidden.shape
    expert_count = lax.axis_size("dp") * w_gate.shape[0]
    return (
        2 * token_count * routes.shape[1] // expert_count >= token_count
        and w_gate.shape[0] == 1
        and lax.axis_size("tp") == 2
        and lax.axis_size("dp") % (CORES * COLUMNS) == 0
        and lax.axis_size("dp") > CORES * COLUMNS
        and token_count % 16 == 0
        and token_count <= LANES
        and half % (PIECES * LANES) == 0
        and w_gate.shape[2] % LANES == 0
    )


def routed_experts(hidden, routes, weights, w_gate, w_up, w_down):
    token_count = hidden.shape[0]
    top_count = routes.shape[1]
    local_experts = w_gate.shape[0]
    expert_count = lax.axis_size("dp") * local_experts
    capacity = min(token_count, 2 * token_count * top_count // expert_count)
    flat_routes = routes.reshape(-1)
    expert_ids = jnp.arange(expert_count, dtype=jnp.int32)
    matches = (flat_routes[:, None] == expert_ids[None, :]).astype(jnp.int32)
    running = jnp.cumsum(matches, axis=0)
    slot_index = jnp.sum(matches * running, axis=1) - 1
    targets = flat_routes * capacity + slot_index
    owners = jnp.arange(token_count * top_count, dtype=jnp.int32) // top_count
    token_table = (
        jnp.full((expert_count * capacity,), token_count, jnp.int32).at[targets].set(owners)
    )
    whole_rows = None
    whole_rows = full_rows(hidden)
    padded = jnp.concatenate(
        [whole_rows, jnp.zeros((1, whole_rows.shape[1]), whole_rows.dtype)], axis=0
    )
    outgoing = jnp.take(padded, token_table, axis=0).reshape(
        expert_count, capacity, whole_rows.shape[1]
    )
    received = lax.all_to_all(outgoing, "dp", split_axis=0, concat_axis=0, tiled=True)
    slot_count = received.shape[1]
    grouped = received.reshape(-1, local_experts, slot_count, received.shape[2])
    gate_act = jnp.einsum("secd,edf->secf", grouped, w_gate, preferred_element_type=jnp.float32)
    upward = jnp.einsum("secd,edf->secf", grouped, w_up, preferred_element_type=jnp.float32)
    active = (jax.nn.silu(gate_act) * upward).astype(jnp.bfloat16)
    partial_value = jnp.einsum("secf,efd->secd", active, w_down, preferred_element_type=jnp.float32)
    partial_value = partial_value.reshape(received.shape[0], slot_count, partial_value.shape[3])
    summed = lax.psum_scatter(
        partial_value.astype(jnp.bfloat16), "tp", scatter_dimension=2, tiled=True
    ).astype(jnp.float32)
    back = lax.all_to_all(
        summed.astype(jnp.bfloat16), "dp", split_axis=0, concat_axis=0, tiled=True
    ).astype(summed.dtype)
    flat_back = back.reshape(expert_count * capacity, back.shape[2])
    picked = jnp.take(flat_back, targets, axis=0).reshape(token_count, top_count, back.shape[2])
    expert_mix = jnp.sum(weights[:, :, None] * picked, axis=1)
    own_out = (hidden.astype(jnp.float32) + expert_mix).astype(jnp.bfloat16)
    full_out = lax.all_gather(own_out, "tp", axis=1, tiled=True)
    return own_out, full_out


def on_device(
    hidden,
    routes,
    routing_weights,
    w_gate,
    w_up,
    w_down,
    norm_gain,
    key_projection_weight,
    value_projection_weight,
    queries,
    cached_key_rows,
    cached_value_rows,
    lengths,
    parents,
):
    token_count = hidden.shape[0]
    expert_count = lax.axis_size("dp") * w_gate.shape[0]
    weights = routing_weights / jnp.sum(routing_weights, axis=1, keepdims=True)
    if dense_fits(hidden, routes, w_gate):
        expert_ids = jnp.arange(expert_count, dtype=jnp.int32)
        named = routes.T[None, :, :] == expert_ids[:, None, None]
        shares = jnp.sum(jnp.where(named, weights.T[None, :, :], 0.0), axis=1)
        shares = jnp.pad(shares, ((0, 0), (0, LANES - token_count)))
        own_out, full_out = dense_experts(hidden, shares, w_gate, w_up, w_down)
    else:
        own_out, full_out = routed_experts(
            hidden, routes, weights, w_gate, w_up, w_down
        )
    widened = full_out.astype(jnp.float32)
    scaling = lax.rsqrt(jnp.mean(widened * widened, axis=1, keepdims=True) + 1e-06)
    normed = (widened * scaling * norm_gain).astype(jnp.bfloat16)
    tree_key_rows = jnp.dot(
        normed, key_projection_weight, preferred_element_type=jnp.float32
    ).astype(jnp.bfloat16)
    tree_value_rows = jnp.dot(
        normed, value_projection_weight, preferred_element_type=jnp.float32
    ).astype(jnp.bfloat16)
    attended = attend_local(
        queries,
        cached_key_rows,
        cached_value_rows,
        tree_key_rows,
        tree_value_rows,
        lengths,
        parents,
    )
    return (own_out, tree_key_rows, tree_value_rows, attended)


def solution(mesh):
    return jax.shard_map(
        on_device,
        mesh=mesh,
        in_specs=(
            P("dp", "tp"),
            P("dp", None),
            P("dp", None),
            P("dp", None, "tp"),
            P("dp", None, "tp"),
            P("dp", "tp", None),
            P(),
            P(None, "tp"),
            P(None, "tp"),
            P("dp", "tp"),
            P("dp", None, "tp"),
            P("dp", None, "tp"),
            P("dp"),
            P("dp", None),
        ),
        out_specs=(P("dp", "tp"), P("dp", "tp"), P("dp", "tp"), P("dp", "tp")),
        check_vma=False,
    )
```
